32 devices in a mesh: row: 4 (over y, x), col: 8 (over z, core).
Axes of the slice: x: 2, y: 2, z: 4, core: 2. Of those that a mesh axis runs over, the one named last changes fastest.
Arguments:
- activations: bfloat16 [1024, 9216], P('col', 'row'), may hold values from -64 to 64
- output_grads: bfloat16 [1024, 73728], P('row', 'col'), may hold values from -16 to 16
- weight: bfloat16 [9216, 73728], P('row', 'col'), may hold values from -1 to 1
- row_moment: float32 [9216], P('row'), may hold values from 0.01 to 0.3
- col_moment: float32 [73728], P('col'), may hold values from 0.01 to 0.3
Outputs:
- new_weight: bfloat16 [9216, 73728], P('row', 'col')
- new_row: float32 [9216], P('row')
- new_col: float32 [73728], P('col')
The draws below stay inside these ranges and needn't reach their ends.
All inputs are finite; a program needn't handle non-finite values.
Results may differ from the reference program's by a relative error of at most 0.0004.
Values may be sent and summed in bfloat16 or wider, within the bound.
A program may use at most 256 MiB of HBM per device.

```python
import math
import jax
import jax.numpy as jnp
from jax import lax

D = 9216
FF = 73728
TOKENS = 1024


def scales(key, length, trend, spread):
    position = jnp.arange(length, dtype=jnp.float32) / length
    jitter = jax.random.uniform(key, (length,), jnp.float32, 0.0, math.log(spread))
    return jnp.exp(math.log(trend) * position + jitter)


def shaped_panel(key, rows_total, width, divisor):
    keys = jax.random.split(key, 2)
    values = jax.random.normal(keys[0], (rows_total, width), jnp.float32)
    factor = scales(keys[1], width, 3.0, 10.0) / 4.0
    return values * factor[None, :] / divisor


def draw_activations(key, part):
    values = shaped_panel(jax.random.fold_in(key, 11), TOKENS, D, 1.0)
    return jnp.clip(values, -64.0, 64.0).astype(jnp.bfloat16)


def draw_output_grads(key, part):
    values = shaped_panel(jax.random.fold_in(key, 23), TOKENS, FF, math.sqrt(TOKENS))
    return jnp.clip(values, -16.0, 16.0).astype(jnp.bfloat16)


def draw_weight(key, part):
    keys = jax.random.split(jax.random.fold_in(key, 37), 3)
    values = jax.random.normal(keys[0], (D, FF), jnp.float32)
    row_scale = scales(keys[1], D, 3.0, 10.0) / 4.0
    col_scale = scales(keys[2], FF, 3.0, 10.0) / 4.0
    values = values * row_scale[:, None] * col_scale[None, :] / math.sqrt(D)
    return jnp.clip(values, -1.0, 1.0).astype(jnp.bfloat16)


def steps_of(key, shape, cuts, low, top_value):
    loudness, own = 1.0, jax.random.fold_in(key, 6)
    for axis_at, shards_of in cuts:
        draws = jnp.exp(jax.random.uniform(jax.random.fold_in(own, axis_at), (shards_of,), jnp.float32, low / len(cuts), top_value / len(cuts)))
        loudness = loudness * jnp.repeat(draws, shape[axis_at] // shards_of).reshape([-1 if axis == axis_at else 1 for axis in range(len(shape))])
    return loudness


def setup_inputs(seed: int = 0) -> dict:
    streams_of = jax.random.split(jax.random.key(seed), 6)
    return {
        "activations": draw_activations(jax.random.fold_in(streams_of[5], 71), 0),
        "output_grads": draw_output_grads(jax.random.fold_in(streams_of[5], 71), 0),
        "weight": draw_weight(jax.random.fold_in(streams_of[5], 71), 0),
        "row_moment": jnp.clip(jnp.exp(math.log(0.3) - 3.4011974 * jax.random.uniform(streams_of[3], (D,), jnp.float32) ** steps_of(streams_of[3], (D,), ((0, 4),), -0.2, 0.2)), 0.01, 0.3),
        "col_moment": jnp.clip(jnp.exp(math.log(0.3) - 3.4011974 * jax.random.uniform(streams_of[4], (FF,), jnp.float32) ** steps_of(streams_of[4], (FF,), ((0, 8),), -0.2, 0.2)), 0.01, 0.3),
    }


ADDED_SQUARE = 1e-30
DECAY_RATE = 0.8
CLIP_LIMIT = 1.0
STEP_SIZE = 0.1
MEAN_OFFSET = 1e-06

def reference(activations, output_grads, weight, row_moment, col_moment):
    block_rows = math.gcd(D, 1152)
    block_count = D // block_rows
    left_side = activations.astype(jnp.float32).T.reshape(block_count, block_rows, TOKENS)
    right_side = output_grads.astype(jnp.float32)
    weight_blocks = weight.reshape(block_count, block_rows, FF)

    def grad_block(left_block):
        return jnp.dot(left_block, right_side, preferred_element_type=jnp.float32)

    def first_pass(carry, left_block):
        squared = jnp.square(grad_block(left_block)) + ADDED_SQUARE
        return (carry + lax.optimization_barrier(jnp.sum(squared, axis=0)), lax.optimization_barrier(jnp.sum(squared, axis=1)))
    col_total, row_total = lax.scan(first_pass, jnp.zeros((FF,), jnp.float32), left_side)
    new_row = DECAY_RATE * row_moment + (1.0 - DECAY_RATE) * row_total.reshape(D) / FF
    new_col = DECAY_RATE * col_moment + (1.0 - DECAY_RATE) * col_total / D
    row_mean = jnp.sum(new_row) / D
    row_blocks = new_row.reshape(block_count, block_rows)

    def update_block(left_block, row_block):
        return grad_block(left_block) / jnp.sqrt(row_block[:, None] * new_col[None, :] / row_mean)

    def second_pass(carry, items):
        left_block, row_block, weight_block = items
        update = update_block(left_block, row_block)
        widened = weight_block.astype(jnp.float32)
        return ((carry[0] + jnp.sum(update * update), carry[1] + jnp.sum(widened * widened)), None)
    start = (jnp.zeros((), jnp.float32), jnp.zeros((), jnp.float32))
    (update_total, weight_total), _ = lax.scan(second_pass, start, (left_side, row_blocks, weight_blocks))
    entries = float(D * FF)
    clip_factor = jnp.maximum(1.0, jnp.sqrt(update_total / entries) / CLIP_LIMIT)
    step_scale = STEP_SIZE * jnp.sqrt(weight_total / entries + MEAN_OFFSET)

    def third_pass(items):
        left_block, row_block, weight_block = items
        update = update_block(left_block, row_block)
        return (weight_block.astype(jnp.float32) - step_scale / clip_factor * update).astype(jnp.bfloat16)
    new_weight = lax.map(third_pass, (left_side, row_blocks, weight_blocks)).reshape(D, FF)
    return (new_weight, new_row, new_col)
```

```python
import functools

import jax
import jax.numpy as jnp
from jax import lax
from jax.experimental import pallas as pl
from jax.experimental.pallas import tpu as pltpu
from jax.sharding import PartitionSpec as P

ADDED_SQUARE = 1e-30
DECAY_RATE = 0.8
CLIP_LIMIT = 1.0
STEP_SIZE = 0.1
MEAN_OFFSET = 1e-06

MESH = pl.DeviceIdType.MESH
WIDTH = 512
PIECES = 3
AHEAD = 3
LAG = 2
SLOTS = LAG + 1
FIXED = 2
KEPT = FIXED + SLOTS
PARTS = 4
WEIGHINGS = 4
W_RING = 3
DOT_PARTS = 2
SPLIT = 2
RING = 5
LOADS = 2
OG_RING = LOADS + 1
ROWS = 256
ACTS_FORWARD = 4
ACTS_READY = 6
GATHER_VMEM = 23800 * 1024
UPDATE_VMEM = 22500 * 1024


def lane_sum(x):
    out = x[:, :128]
    for k in range(1, x.shape[1] // 128):
        out = out + x[:, k * 128 : (k + 1) * 128]
    return out


def sublane_sum(x):
    return jnp.sum(x.reshape(x.shape[0] // 8, 8, x.shape[1]), axis=0)


def slot_of(k):
    return jnp.where(k < FIXED, k, FIXED + lax.rem(k - FIXED + FIXED * SLOTS, SLOTS))


def chunk_in(s, n):
    base = n - SLOTS
    return jnp.where(s < FIXED, s, base + lax.rem(s + SLOTS * n - base, SLOTS))


def gather_kernel(
    rows, cols,
    acts_ref, og_ref, w_ref, rm_ref, cm_ref, *refs,
):
    og_out, nr_out, nc_out, rs_out, cs_out, *refs = refs
    acts_t, refs = refs[:PIECES], refs[PIECES:]
    grad, refs = refs[: PIECES * PARTS], refs[PIECES * PARTS :]
    og_all, wbuf, rowacc, wacc, colx, rowx, scb, scc, *sems = refs
    load_sem, og_sem, acts_sem, sib_sem, col_sem, row_sem, scb_sem, scc_sem, w_sem, misc_sem, out_sem = sems
    n, tokens, width = og_all.shape
    sub = acts_t[0].shape[0]
    tile_rows = sub * PIECES
    thin = sub // PARTS
    part = acts_ref.shape[0]
    spans = -(-tile_rows // width)
    shared = -(-spans // 2)
    share = tokens // rows
    half = share // 2
    wrows = wbuf.shape[1]
    sacc = rs_out
    total_rows = tile_rows * rows
    total_cols = n * width * cols
    entries = float(total_rows * total_cols)
    r, c = lax.axis_index("row"), lax.axis_index("col")
    rx = r + 1 - 2 * lax.rem(r, 2)
    ry = lax.rem(r + 2, 4)
    rd = lax.rem(rx + 2, 4)
    sib = c + 1 - 2 * lax.rem(c, 2)

    def region(owner, start, size):
        return pl.ds(pl.multiple_of(owner * share + start, half), size)

    def load(j):
        return pltpu.make_async_copy(
            og_ref.at[:, pl.ds(pl.multiple_of(j * width, width), width)],
            og_all.at[j, region(r, 0, share), :], load_sem.at[j])

    def og_copy(j, kind, owner, start, size, to):
        ref = og_all.at[j, region(owner, start, size), :]
        return pltpu.make_async_remote_copy(
            src_ref=ref, dst_ref=ref, send_sem=og_sem.at[0, kind, j], recv_sem=og_sem.at[1, kind, j],
            device_id={"row": to}, device_id_type=MESH)

    def own_x(j):
        return og_copy(j, 0, r, 0, share, rx)

    def own_y(j):
        return og_copy(j, 1, r, 0, share, ry)

    def fwd_y(j):
        return og_copy(j, 2, rx, 0, half, ry)

    def fwd_x(j):
        return og_copy(j, 3, ry, half, half, rx)

    def acts_part(i, q):
        return acts_t[i].at[:, pl.ds(pl.multiple_of(q * part, part), part)]

    def acts_copies(d):
        to = lax.rem(c + 2 * d, cols)
        return [pltpu.make_async_remote_copy(
            src_ref=acts_part(i, c), dst_ref=acts_part(i, c),
            send_sem=acts_sem.at[0, d, i], recv_sem=acts_sem.at[1, d, i],
            device_id={"col": to}, device_id_type=MESH) for i in range(PIECES)]

    def sib_copies(d):
        at = lax.rem(c + cols - 2 * d, cols)
        return [pltpu.make_async_remote_copy(
            src_ref=acts_part(i, at), dst_ref=acts_part(i, at),
            send_sem=sib_sem.at[0, d, i], recv_sem=sib_sem.at[1, d, i],
            device_id={"col": sib}, device_id_type=MESH) for i in range(PIECES)]

    def col_copy(j, d):
        return pltpu.make_async_remote_copy(
            src_ref=colx.at[r, j], dst_ref=colx.at[r, j], send_sem=col_sem.at[0, d, j], recv_sem=col_sem.at[1, d, j],
            device_id={"row": lax.rem(r + d, rows)}, device_id_type=MESH)

    def row_copy(d):
        return pltpu.make_async_remote_copy(
            src_ref=rowx.at[c], dst_ref=rowx.at[c], send_sem=row_sem.at[0, d], recv_sem=row_sem.at[1, d],
            device_id={"col": lax.rem(c + d, cols)}, device_id_type=MESH)

    def scb_copy(d):
        return pltpu.make_async_remote_copy(
            src_ref=scb.at[c], dst_ref=scb.at[c], send_sem=scb_sem.at[0, d], recv_sem=scb_sem.at[1, d],
            device_id={"col": lax.rem(c + d, cols)}, device_id_type=MESH)

    def scc_copy(d):
        return pltpu.make_async_remote_copy(
            src_ref=scc.at[r], dst_ref=scc.at[r], send_sem=scc_sem.at[0, d], recv_sem=scc_sem.at[1, d],
            device_id={"row": lax.rem(r + d, rows)}, device_id_type=MESH)

    def w_copy(j):
        return pltpu.make_async_copy(
            w_ref.at[pl.ds(pl.multiple_of(j * wrows, wrows), wrows), :], wbuf.at[lax.rem(j, W_RING)], w_sem.at[lax.rem(j, W_RING)])

    def og_store(j):
        return pltpu.make_async_copy(og_all.at[j], og_out.at[j], out_sem.at[j])

    def acts_span(m):
        return n - 1 - m // 2, pl.ds(pl.multiple_of(r * share + m % 2 * part, part), part), min(width, tile_rows - m * width)

    def acts_load(m):
        slab, at, lanes = acts_span(m)
        return pltpu.make_async_copy(
            acts_ref.at[:, pl.ds(m * width, lanes)], og_all.at[slab, at, pl.ds(0, lanes)], misc_sem.at[m])


    for m in range(spans):
        acts_load(m).start()

    @pl.loop(0, n - shared)
    def _(j):
        load(j).start()

    for j in range(W_RING):
        w_copy(j).start()

    barrier = pltpu.get_barrier_semaphore()
    for d in range(1, rows):
        pl.semaphore_signal(barrier, inc=1, device_id={"row": lax.rem(r + d, rows)}, device_id_type=MESH)
    for d in range(1, cols):
        pl.semaphore_signal(barrier, inc=1, device_id={"col": lax.rem(c + d, cols)}, device_id_type=MESH)
    rowacc[...] = jnp.zeros_like(rowacc)
    sacc[...] = jnp.zeros_like(sacc)
    wacc[...] = jnp.zeros_like(wacc)
    own = pl.ds(pl.multiple_of(c * part, part), part)
    for m in range(spans):
        acts_load(m).wait()
        slab, at, lanes = acts_span(m)
        for o in range(0, lanes, ROWS):
            i, low = divmod(m * width + o, sub)
            acts_t[i][low : low + ROWS, own] = og_all[slab, at, o : o + ROWS].T

    @pl.loop(n - shared, n)
    def _(j):
        load(j).start()

    pl.semaphore_wait(barrier, rows + cols - 2)

    def send_own(j):
        load(j).wait()
        own_x(j).start()
        own_y(j).start()

    for j in range(AHEAD):
        send_own(j)
    for d in range(1, cols // 2):
        for copy in acts_copies(d):
            copy.start()
    for copy in sib_copies(0):
        copy.start()

    def exchange(j):
        own_x(j).wait_recv()
        fwd_y(j).start()
        own_y(j).wait_recv()
        fwd_x(j).start()

        @pl.when(j + AHEAD < n)
        def _():
            send_own(j + AHEAD)

    def weigh(j):
        @pl.loop(j * WEIGHINGS, (j + 1) * WEIGHINGS)
        def _(k):
            weigh_rows(k)

    def weigh_rows(j):
        w_copy(j).wait()
        s = lax.rem(j, W_RING)
        wide = 1024

        @pl.loop(0, wbuf.shape[2] // wide)
        def _(k):
            x = wbuf[s, :, pl.ds(pl.multiple_of(k * wide, wide), wide)].astype(jnp.float32)
            wacc[...] += sublane_sum(x * x)

        @pl.when(j + W_RING < n * WEIGHINGS)
        def _():
            w_copy(j + W_RING).start()

    def stats(k):
        for d in range(1, rows):
            col_copy(k, d).wait_recv()
        total = colx[0, k]
        for q in range(1, rows):
            total = total + colx[q, k]
        factor = DECAY_RATE * cm_ref[k] + (1.0 - DECAY_RATE) * total / total_rows
        nc_out[k] = factor
        cs_out[k] = lax.rsqrt(factor)
        weight = 1.0 / factor
        s = slot_of(k)

        for i in range(PIECES * PARTS):
            g = grad[i][s]
            sacc[pl.ds(i * thin, thin), :] += lane_sum(g * g * weight)

    def compute(k):
        fwd_y(k).wait_recv()
        fwd_x(k).wait_recv()
        s = slot_of(k)
        @pl.when((k >= FIXED) & (k < n - SLOTS))
        def _():
            og_store(k).start()

        right = og_all.at[k]
        column = jnp.zeros((8, width), jnp.float32)
        tall = thin * DOT_PARTS
        for row in range(0, tile_rows, tall):
            i, low = divmod(row, sub)
            g = jnp.dot(acts_t[i][low : low + tall, :], right[...], preferred_element_type=jnp.float32)
            for p in range(DOT_PARTS):
                grad[row // thin + p][s] = g[p * thin : (p + 1) * thin]
            squared = g * g + ADDED_SQUARE
            rowacc[pl.ds(row, tall), :] += lane_sum(squared)
            column = column + sublane_sum(squared)
        colx[r, k] = jnp.sum(column, axis=0, keepdims=True)
        for d in range(1, rows):
            col_copy(k, d).start()

        @pl.when(k >= LAG)
        def _():
            stats(k - LAG)

    def reach(j):
        return jnp.minimum(j, 2 * (j - ACTS_READY + 1))

    @pl.loop(0, ACTS_FORWARD)
    def _(j):
        exchange(j)
        weigh(j)

    for d in range(1, cols // 2):
        for copy, onward in zip(acts_copies(d), sib_copies(d)):
            copy.wait_recv()
            onward.start()

    @pl.loop(ACTS_FORWARD, ACTS_READY)
    def _(j):
        exchange(j)
        weigh(j)

    for d in range(cols // 2):
        for copy in sib_copies(d):
            copy.wait_recv()

    @pl.loop(ACTS_READY, n)
    def _(j):
        exchange(j)
        weigh(j)

        @pl.loop(reach(j - 1), reach(j))
        def _(k):
            compute(k)

    @pl.loop(n - 1, n)
    def _(k):
        compute(k)

    rowx[c] = jnp.sum(rowacc[...].T, axis=0, keepdims=True)
    for d in range(1, cols):
        row_copy(d).start()

    @pl.loop(n - LAG, n)
    def _(k):
        stats(k)

    ratio_rows = jnp.sum(sacc[...].T, axis=0, keepdims=True)
    for d in range(1, cols):
        row_copy(d).wait_recv()
    row_total = rowx[0]
    for q in range(1, cols):
        row_total = row_total + rowx[q]
    new_row = DECAY_RATE * rm_ref[...] + (1.0 - DECAY_RATE) * row_total / total_cols
    nr_out[...] = new_row

    def spread(x):
        return jnp.broadcast_to(jnp.sum(x, axis=1, keepdims=True), (1, 128))

    scb[c, 0:1, :] = spread(ratio_rows / new_row)
    scb[c, 1:2, :] = spread(jnp.sum(wacc[...], axis=0, keepdims=True))
    for d in range(1, cols):
        scb_copy(d).start()
    row_sum = spread(new_row)
    for d in range(1, cols):
        scb_copy(d).wait_recv()
    both = scb[0]
    for q in range(1, cols):
        both = both + scb[q]
    scc[r, 0:2, :] = both[0:2, :]
    scc[r, 2:3, :] = row_sum
    for d in range(1, rows):
        scc_copy(d).start()
    root = lax.rsqrt(new_row)
    for d in range(1, rows):
        scc_copy(d).wait_recv()
    every = scc[0]
    for q in range(1, rows):
        every = every + scc[q]
    row_mean = every[2:3, :] / total_rows
    rms_update = jnp.sqrt(row_mean * (every[0:1, :] / entries))
    clip_factor = jnp.maximum(1.0, rms_update / CLIP_LIMIT)
    step_scale = STEP_SIZE * jnp.sqrt(every[1:2, :] / entries + MEAN_OFFSET)
    scale = step_scale / clip_factor * jnp.sqrt(row_mean)
    rs_out[...] = jnp.broadcast_to(root, (128, tile_rows)).T * scale

    @pl.loop(0, n)
    def _(j):
        own_x(j).wait_send()
        own_y(j).wait_send()
        fwd_y(j).wait_send()
        fwd_x(j).wait_send()
        for d in range(1, rows):
            col_copy(j, d).wait_send()

    @pl.loop(FIXED, n - SLOTS)
    def _(j):
        og_store(j).wait()

    for d in range(1, cols // 2):
        for copy in acts_copies(d):
            copy.wait_send()
    for d in range(cols // 2):
        for copy in sib_copies(d):
            copy.wait_send()
    for d in range(1, cols):
        row_copy(d).wait_send()
        scb_copy(d).wait_send()
    for d in range(1, rows):
        scc_copy(d).wait_send()


def update_kernel(og_ref, w_ref, rs_ref, cs_ref, *refs):
    acts_t, refs = refs[:PIECES], refs[PIECES:]
    grad, refs = refs[: PIECES * PARTS], refs[PIECES * PARTS :]
    out_ref, og_buf, made_buf, kept_buf, og_sem, in_sem, out_sem = refs
    n, _, width = og_ref.shape
    sub = acts_t[0].shape[0]
    thin = sub // PARTS
    narrow = width // SPLIT
    chunks = n - KEPT

    def og_load(t):
        return pltpu.make_async_copy(og_ref.at[FIXED + t], og_buf.at[lax.rem(t, OG_RING)], og_sem.at[lax.rem(t, OG_RING)])

    def copies(t, out):
        b = lax.rem(t, RING)
        made = pl.ds(pl.multiple_of((FIXED + t) * width, width), width)
        kept = pl.ds(pl.multiple_of(chunk_in(lax.div(t, SPLIT), n) * width + lax.rem(t, SPLIT) * narrow, narrow), narrow)
        if out:
            return (pltpu.make_async_copy(made_buf.at[b], out_ref.at[:, made], out_sem.at[0, b]),
                    pltpu.make_async_copy(kept_buf.at[b], out_ref.at[:, kept], out_sem.at[1, b]))
        return (pltpu.make_async_copy(w_ref.at[:, made], made_buf.at[b], in_sem.at[0, b]),
                pltpu.make_async_copy(w_ref.at[:, kept], kept_buf.at[b], in_sem.at[1, b]))

    def finish(g, w, row, cs):
        rs = rs_ref[pl.ds(row, g.shape[0]), :]
        wide = jnp.concatenate([rs] * (g.shape[1] // 128), axis=1)
        return (w.astype(jnp.float32) - g * wide * cs).astype(w.dtype)

    mixed = KEPT * SPLIT

    def each(t, out, act):
        made, kept = copies(t, out)
        act(made)

        @pl.when(t < mixed)
        def _():
            act(kept)

    def start(copy):
        copy.start()

    def wait(copy):
        copy.wait()

    for t in range(LOADS):
        og_load(t).start()
        each(t, False, start)

    def body(t, mix):
        b = lax.rem(t, RING)

        @pl.when(t >= RING - LOADS)
        def _():
            each(t - (RING - LOADS), True, wait)

        @pl.when(t + LOADS < chunks)
        def _():
            og_load(t + LOADS).start()
            each(t + LOADS, False, start)

        og_load(t).wait()
        each(t, False, wait)
        right = og_buf.at[lax.rem(t, OG_RING)]
        s = lax.div(t, SPLIT)
        lanes = pl.ds(pl.multiple_of(lax.rem(t, SPLIT) * narrow, narrow), narrow)
        made_cs = cs_ref[FIXED + t]
        kept_cs = cs_ref[chunk_in(s, n), :, lanes] if mix else None

        def make(row):
            i, low = row // sub, row % sub
            left = acts_t[i][low : low + ROWS, :]
            return row, jnp.dot(left, right[...], preferred_element_type=jnp.float32)

        def settle(row, g):
            at = pl.ds(row, ROWS)
            made_buf[b, at, :] = finish(g, made_buf[b, at, :], row, made_cs)

        def keep(p):
            at = pl.ds(p * thin, thin)
            kept_buf[b, at, :] = finish(grad[p][s, :, lanes], kept_buf[b, at, :], p * thin, kept_cs)

        blocks = sub * PIECES // ROWS
        parts = PIECES * PARTS
        last = None
        for k in range(blocks):
            g = make(k * ROWS)
            for p in range(k * parts // blocks, (k + 1) * parts // blocks) if mix else ():
                keep(p)
            if last is not None:
                settle(*last)
            last = g
        settle(*last)
        each(t, True, start)

    @pl.loop(0, mixed)
    def _(t):
        body(t, True)

    @pl.loop(mixed, chunks)
    def _(t):
        body(t, False)

    @pl.loop(chunks - (RING - LOADS), chunks)
    def _(t):
        each(t, True, wait)


def with_kernels(rows, cols, activations, output_grads, weight, row_moment, col_moment):
    tile_rows, tile_cols = weight.shape
    part = activations.shape[0]
    tokens = part * cols
    n, width = tile_cols // WIDTH, WIDTH
    f32, bf16 = jnp.float32, jnp.bfloat16
    any_space = pl.BlockSpec(memory_space=pl.ANY)
    vmem = pl.BlockSpec(memory_space=pltpu.VMEM)
    dma = pltpu.SemaphoreType.DMA
    flops = 2 * tile_rows * tile_cols * tokens
    sub = tile_rows // PIECES
    activations, output_grads, weight = (
        pltpu.with_memory_space_constraint(x, pltpu.HBM) for x in (activations, output_grads, weight))
    og_all, new_row, new_col, *inner = pl.pallas_call(
        functools.partial(gather_kernel, rows, cols),
        out_shape=(
            pltpu.HBM((n, tokens, width), bf16),
            jax.ShapeDtypeStruct((1, tile_rows), f32),
            jax.ShapeDtypeStruct((n, 1, width), f32),
            jax.ShapeDtypeStruct((tile_rows, 128), f32),
            jax.ShapeDtypeStruct((n, 1, width), f32),
            *([jax.ShapeDtypeStruct((sub, tokens), bf16)] * PIECES),
            *([jax.ShapeDtypeStruct((KEPT, sub // PARTS, width), f32)] * (PIECES * PARTS)),
        ),
        in_specs=[any_space, any_space, any_space, vmem, vmem],
        out_specs=(any_space,) + (vmem,) * (4 + PIECES + PIECES * PARTS),
        scratch_shapes=[
            pltpu.VMEM((n, tokens, width), bf16),
            pltpu.VMEM((W_RING, tile_rows // (n * WEIGHINGS), tile_cols), bf16),
            pltpu.VMEM((tile_rows, 128), f32),
            pltpu.VMEM((8, 1024), f32),
            pltpu.VMEM((rows, n, 1, width), f32),
            pltpu.VMEM((cols, 1, tile_rows), f32),
            pltpu.VMEM((cols, 2, 128), f32),
            pltpu.VMEM((rows, 3, 128), f32),
            dma((n,)), dma((2, 4, n)), dma((2, cols // 2, PIECES)), dma((2, cols // 2, PIECES)), dma((2, rows, n)),
            dma((2, cols)), dma((2, cols)), dma((2, rows)), dma((W_RING,)), dma((-(-tile_rows // width),)), dma((n,)),
        ],
        compiler_params=pltpu.CompilerParams(
            collective_id=0, has_side_effects=True, vmem_limit_bytes=GATHER_VMEM),
        cost_estimate=pl.CostEstimate(flops=flops, bytes_accessed=2 * weight.size, transcendentals=0),
        name="gather_stats",
    )(activations, output_grads, weight, row_moment.reshape(1, tile_rows), col_moment.reshape(n, 1, width))
    og_all = pltpu.with_memory_space_constraint(og_all, pltpu.HBM)
    new_weight = pl.pallas_call(
        update_kernel,
        out_shape=jax.ShapeDtypeStruct((tile_rows, tile_cols), bf16),
        in_specs=[any_space, any_space] + [vmem] * len(inner),
        out_specs=any_space,
        scratch_shapes=[
            pltpu.VMEM((OG_RING, tokens, width), bf16),
            pltpu.VMEM((RING, tile_rows, width), bf16),
            pltpu.VMEM((RING, tile_rows, width // SPLIT), bf16),
            dma((OG_RING,)), dma((2, RING)), dma((2, RING)),
        ],
        compiler_params=pltpu.CompilerParams(vmem_limit_bytes=UPDATE_VMEM),
        cost_estimate=pl.CostEstimate(flops=flops, bytes_accessed=4 * weight.size, transcendentals=0),
        name="update_weight",
    )(og_all, weight, *inner)
    return new_weight, new_row.reshape(tile_rows), new_col.reshape(tile_cols)


def plain(activations, output_grads, weight, row_moment, col_moment):
    tile_rows, tile_cols = weight.shape
    total_rows = tile_rows * lax.axis_size("row")
    total_cols = tile_cols * lax.axis_size("col")
    entries = float(total_rows * total_cols)
    weight_wide = weight.astype(jnp.float32)
    weight_local = jnp.sum(weight_wide * weight_wide)
    weight_total = lax.psum(weight_local, ("row", "col"))
    contract = (((0,), (0,)), ((), ()))
    acts_all = lax.all_gather(activations, "col", axis=0, tiled=True)
    gradient = lax.dot_general(
        acts_all,
        lax.all_gather(output_grads, "row", axis=0, tiled=True),
        contract,
        preferred_element_type=jnp.float32,
    )
    squared = gradient * gradient
    row_part = jnp.sum(squared + ADDED_SQUARE, axis=1)
    col_part = jnp.sum(squared + ADDED_SQUARE, axis=0)
    row_total = lax.psum(row_part, "col")
    col_total = lax.psum(col_part, "row")
    new_row = DECAY_RATE * row_moment + (1.0 - DECAY_RATE) * row_total / total_cols
    new_col = DECAY_RATE * col_moment + (1.0 - DECAY_RATE) * col_total / total_rows
    inverse = lax.rsqrt(new_row[:, None] * new_col[None, :])
    ratio_local = jnp.sum(squared * inverse * inverse)
    leader = (lax.axis_index("col") == 0).astype(jnp.float32)
    row_local = leader * jnp.sum(new_row)
    row_sum, ratio_sum = lax.psum((row_local, ratio_local), ("row", "col"))
    row_mean = row_sum / total_rows
    rms_update = jnp.sqrt(row_mean * ratio_sum / entries)
    clip_factor = jnp.maximum(1.0, rms_update / CLIP_LIMIT)
    step_scale = STEP_SIZE * jnp.sqrt(weight_total / entries + MEAN_OFFSET)
    update = gradient * inverse * jnp.sqrt(row_mean)
    new_weight = (weight_wide - step_scale / clip_factor * update).astype(jnp.bfloat16)
    return (new_weight, new_row, new_col)


def on_device(rows, cols, activations, output_grads, weight, row_moment, col_moment):
    tile_rows, tile_cols = weight.shape
    chunks = tile_cols // WIDTH
    fits = (
        rows == 4 and cols % 2 == 0 and cols > 2
        and tile_rows % (64 * PIECES * PARTS) == 0 and tile_rows % (PIECES * ROWS) == 0 and tile_cols % 1024 == 0
        and chunks > max(ACTS_READY, KEPT) + SLOTS and tile_rows % (8 * chunks * WEIGHINGS) == 0
        and chunks >= KEPT * (SPLIT + 1) and tile_rows % ROWS == 0 and 2 * activations.shape[0] <= output_grads.shape[0]
        and output_grads.shape[0] % 32 == 0 and activations.shape[0] % 128 == 0
    )
    args = (activations, output_grads, weight, row_moment, col_moment)
    return with_kernels(rows, cols, *args) if fits else plain(*args)


def solution(mesh):
    return jax.shard_map(
        functools.partial(on_device, mesh.shape["row"], mesh.shape["col"]),
        mesh=mesh,
        in_specs=(P("col", "row"), P("row", "col"), P("row", "col"), P("row"), P("col")),
        out_specs=(P("row", "col"), P("row"), P("col")),
        check_vma=False,
    )
```

```python
import functools

import jax
import jax.numpy as jnp
from jax import lax
from jax.experimental import pallas as pl
from jax.experimental.pallas import tpu as pltpu
from jax.sharding import PartitionSpec as P

ADDED_SQUARE = 1e-30
DECAY_RATE = 0.8
CLIP_LIMIT = 1.0
STEP_SIZE = 0.1
MEAN_OFFSET = 1e-06

MESH = pl.DeviceIdType.MESH
WIDTH = 512
PIECES = 3
AHEAD = 3
LAG = 2
SLOTS = LAG + 1
FIXED = 2
KEPT = FIXED + SLOTS
PARTS = 4
WEIGHINGS = 4
W_RING = 3
DOT_PARTS = 2
SPLIT = 2
RING = 5
LOADS = 2
OG_RING = LOADS + 1
ROWS = 256
ACTS_FORWARD = 4
ACTS_READY = 6
GATHER_VMEM = 23800 * 1024
UPDATE_VMEM = 22500 * 1024


def lane_sum(x):
    out = x[:, :128]
    for k in range(1, x.shape[1] // 128):
        out = out + x[:, k * 128 : (k + 1) * 128]
    return out


def sublane_sum(x):
    return jnp.sum(x.reshape(x.shape[0] // 8, 8, x.shape[1]), axis=0)


def slot_of(k):
    return jnp.where(k < FIXED, k, FIXED + lax.rem(k - FIXED + FIXED * SLOTS, SLOTS))


def chunk_in(s, n):
    base = n - SLOTS
    return jnp.where(s < FIXED, s, base + lax.rem(s + SLOTS * n - base, SLOTS))


def gather_kernel(
    rows, cols,
    acts_ref, og_ref, w_ref, rm_ref, cm_ref, *refs,
):
    og_out, nr_out, nc_out, rs_out, cs_out, *refs = refs
    acts_t, refs = refs[:PIECES], refs[PIECES:]
    grad, refs = refs[: PIECES * PARTS], refs[PIECES * PARTS :]
    og_all, wbuf, rowacc, wacc, colx, rowx, scb, scc, *sems = refs
    load_sem, og_sem, acts_sem, sib_sem, col_sem, row_sem, scb_sem, scc_sem, w_sem, misc_sem, out_sem = sems
    n, tokens, width = og_all.shape
    sub = acts_t[0].shape[0]
    tile_rows = sub * PIECES
    thin = sub // PARTS
    part = acts_ref.shape[0]
    spans = -(-tile_rows // width)
    shared = -(-spans // 2)
    share = tokens // rows
    half = share // 2
    wrows = wbuf.shape[1]
    sacc = rs_out
    total_rows = tile_rows * rows
    total_cols = n * width * cols
    entries = float(total_rows * total_cols)
    r, c = lax.axis_index("row"), lax.axis_index("col")
    rx = r + 1 - 2 * lax.rem(r, 2)
    ry = lax.rem(r + 2, 4)
    rd = lax.rem(rx + 2, 4)
    sib = c + 1 - 2 * lax.rem(c, 2)

    def region(owner, start, size):
        return pl.ds(pl.multiple_of(owner * share + start, half), size)

    def load(j):
        return pltpu.make_async_copy(
            og_ref.at[:, pl.ds(pl.multiple_of(j * width, width), width)],
            og_all.at[j, region(r, 0, share), :], load_sem.at[j])

    def og_copy(j, kind, owner, start, size, to):
        ref = og_all.at[j, region(owner, start, size), :]
        return pltpu.make_async_remote_copy(
            src_ref=ref, dst_ref=ref, send_sem=og_sem.at[0, kind, j], recv_sem=og_sem.at[1, kind, j],
            device_id={"row": to}, device_id_type=MESH)

    def own_x(j):
        return og_copy(j, 0, r, 0, share, rx)

    def own_y(j):
        return og_copy(j, 1, r, 0, share, ry)

    def fwd_y(j):
        return og_copy(j, 2, rx, 0, half, ry)

    def fwd_x(j):
        return og_copy(j, 3, ry, half, half, rx)

    def acts_part(i, q):
        return acts_t[i].at[:, pl.ds(pl.multiple_of(q * part, part), part)]

    def acts_copies(d):
        to = lax.rem(c + 2 * d, cols)
        return [pltpu.make_async_remote_copy(
            src_ref=acts_part(i, c), dst_ref=acts_part(i, c),
            send_sem=acts_sem.at[0, d, i], recv_sem=acts_sem.at[1, d, i],
            device_id={"col": to}, device_id_type=MESH) for i in range(PIECES)]

    def sib_copies(d):
        at = lax.rem(c + cols - 2 * d, cols)
        return [pltpu.make_async_remote_copy(
            src_ref=acts_part(i, at), dst_ref=acts_part(i, at),
            send_sem=sib_sem.at[0, d, i], recv_sem=sib_sem.at[1, d, i],
            device_id={"col": sib}, device_id_type=MESH) for i in range(PIECES)]

    def col_copy(j, d):
        return pltpu.make_async_remote_copy(
            src_ref=colx.at[r, j], dst_ref=colx.at[r, j], send_sem=col_sem.at[0, d, j], recv_sem=col_sem.at[1, d, j],
            device_id={"row": lax.rem(r + d, rows)}, device_id_type=MESH)

    def row_copy(d):
        return pltpu.make_async_remote_copy(
            src_ref=rowx.at[c], dst_ref=rowx.at[c], send_sem=row_sem.at[0, d], recv_sem=row_sem.at[1, d],
            device_id={"col": lax.rem(c + d, cols)}, device_id_type=MESH)

    def scb_copy(d):
        return pltpu.make_async_remote_copy(
            src_ref=scb.at[c], dst_ref=scb.at[c], send_sem=scb_sem.at[0, d], recv_sem=scb_sem.at[1, d],
            device_id={"col": lax.rem(c + d, cols)}, device_id_type=MESH)

    def scc_copy(d):
        return pltpu.make_async_remote_copy(
            src_ref=scc.at[r], dst_ref=scc.at[r], send_sem=scc_sem.at[0, d], recv_sem=scc_sem.at[1, d],
            device_id={"row": lax.rem(r + d, rows)}, device_id_type=MESH)

    def w_copy(j):
        return pltpu.make_async_copy(
            w_ref.at[pl.ds(pl.multiple_of(j * wrows, wrows), wrows), :], wbuf.at[lax.rem(j, W_RING)], w_sem.at[lax.rem(j, W_RING)])

    def og_store(j):
        return pltpu.make_async_copy(og_all.at[j], og_out.at[j], out_sem.at[j])

    def acts_span(m):
        return n - 1 - m // 2, pl.ds(pl.multiple_of(r * share + m % 2 * part, part), part), min(width, tile_rows - m * width)

    def acts_load(m):
        slab, at, lanes = acts_span(m)
        return pltpu.make_async_copy(
            acts_ref.at[:, pl.ds(m * width, lanes)], og_all.at[slab, at, pl.ds(0, lanes)], misc_sem.at[m])


    for m in range(spans):
        acts_load(m).start()

    @pl.loop(0, n - shared)
    def _(j):
        load(j).start()

    for j in range(W_RING):
        w_copy(j).start()

    barrier = pltpu.get_barrier_semaphore()
    for d in range(1, rows):
        pl.semaphore_signal(barrier, inc=1, device_id={"row": lax.rem(r + d, rows)}, device_id_type=MESH)
    for d in range(1, cols):
        pl.semaphore_signal(barrier, inc=1, device_id={"col": lax.rem(c + d, cols)}, device_id_type=MESH)
    rowacc[...] = jnp.zeros_like(rowacc)
    sacc[...] = jnp.zeros_like(sacc)
    wacc[...] = jnp.zeros_like(wacc)
    own = pl.ds(pl.multiple_of(c * part, part), part)
    for m in range(spans):
        acts_load(m).wait()
        slab, at, lanes = acts_span(m)
        for o in range(0, lanes, ROWS):
            i, low = divmod(m * width + o, sub)
            acts_t[i][low : low + ROWS, own] = og_all[slab, at, o : o + ROWS].T

    @pl.loop(n - shared, n)
    def _(j):
        load(j).start()

    pl.semaphore_wait(barrier, rows + cols - 2)

    def send_own(j):
        load(j).wait()
        own_x(j).start()
        own_y(j).start()

    for j in range(AHEAD):
        send_own(j)
    for d in range(1, cols // 2):
        for copy in acts_copies(d):
            copy.start()
    for copy in sib_copies(0):
        copy.start()

    def exchange(j):
        own_x(j).wait_recv()
        fwd_y(j).start()
        own_y(j).wait_recv()
        fwd_x(j).start()

        @pl.when(j + AHEAD < n)
        def _():
            send_own(j + AHEAD)

    def weigh(j):
        @pl.loop(j * WEIGHINGS, (j + 1) * WEIGHINGS)
        def _(k):
            weigh_rows(k)

    def weigh_rows(j):
        w_copy(j).wait()
        s = lax.rem(j, W_RING)
        wide = 1024

        @pl.loop(0, wbuf.shape[2] // wide)
        def _(k):
            x = wbuf[s, :, pl.ds(pl.multiple_of(k * wide, wide), wide)].astype(jnp.float32)
            wacc[...] += sublane_sum(x * x)

        @pl.when(j + W_RING < n * WEIGHINGS)
        def _():
            w_copy(j + W_RING).start()

    def stats(k):
        for d in range(1, rows):
            col_copy(k, d).wait_recv()
        total = colx[0, k]
        for q in range(1, rows):
            total = total + colx[q, k]
        factor = DECAY_RATE * cm_ref[k] + (1.0 - DECAY_RATE) * total / total_rows
        nc_out[k] = factor
        cs_out[k] = lax.rsqrt(factor)
        weight = 1.0 / factor
        s = slot_of(k)

        for i in range(PIECES * PARTS):
            g = grad[i][s]
            sacc[pl.ds(i * thin, thin), :] += lane_sum(g * g * weight)

    def compute(k):
        fwd_y(k).wait_recv()
        fwd_x(k).wait_recv()
        s = slot_of(k)
        @pl.when((k >= FIXED) & (k < n - SLOTS))
        def _():
            og_store(k).start()

        right = og_all.at[k]
        column = jnp.zeros((8, width), jnp.float32)
        tall = thin * DOT_PARTS
        for row in range(0, tile_rows, tall):
            i, low = divmod(row, sub)
            g = jnp.dot(acts_t[i][low : low + tall, :], right[...], preferred_element_type=jnp.float32)
            for p in range(DOT_PARTS):
                grad[row // thin + p][s] = g[p * thin : (p + 1) * thin]
            squared = g * g + ADDED_SQUARE
            rowacc[pl.ds(row, tall), :] += lane_sum(squared)
            column = column + sublane_sum(squared)
        colx[r, k] = jnp.sum(column, axis=0, keepdims=True)
        for d in range(1, rows):
            col_copy(k, d).start()

        @pl.when(k >= LAG)
        def _():
            stats(k - LAG)

    def reach(j):
        return jnp.minimum(j, 2 * (j - ACTS_READY + 1))

    @pl.loop(0, ACTS_FORWARD)
    def _(j):
        exchange(j)
        weigh(2 * j)
        weigh(2 * j + 1)

    for d in range(1, cols // 2):
        for copy, onward in zip(acts_copies(d), sib_copies(d)):
            copy.wait_recv()
            onward.start()

    @pl.loop(ACTS_FORWARD, ACTS_READY)
    def _(j):
        exchange(j)
        weigh(2 * j)
        weigh(2 * j + 1)

    for d in range(cols // 2):
        for copy in sib_copies(d):
            copy.wait_recv()

    @pl.loop(ACTS_READY, n)
    def _(j):
        exchange(j)

        @pl.when(j >= 2 * ACTS_READY)
        def _():
            weigh(j)

        @pl.loop(reach(j - 1), reach(j))
        def _(k):
            compute(k)

    @pl.loop(n - 1, n)
    def _(k):
        compute(k)

    rowx[c] = jnp.sum(rowacc[...].T, axis=0, keepdims=True)
    for d in range(1, cols):
        row_copy(d).start()

    @pl.loop(n - LAG, n)
    def _(k):
        stats(k)

    ratio_rows = jnp.sum(sacc[...].T, axis=0, keepdims=True)
    for d in range(1, cols):
        row_copy(d).wait_recv()
    row_total = rowx[0]
    for q in range(1, cols):
        row_total = row_total + rowx[q]
    new_row = DECAY_RATE * rm_ref[...] + (1.0 - DECAY_RATE) * row_total / total_cols
    nr_out[...] = new_row

    def spread(x):
        return jnp.broadcast_to(jnp.sum(x, axis=1, keepdims=True), (1, 128))

    scb[c, 0:1, :] = spread(ratio_rows / new_row)
    scb[c, 1:2, :] = spread(jnp.sum(wacc[...], axis=0, keepdims=True))
    for d in range(1, cols):
        scb_copy(d).start()
    row_sum = spread(new_row)
    for d in range(1, cols):
        scb_copy(d).wait_recv()
    both = scb[0]
    for q in range(1, cols):
        both = both + scb[q]
    scc[r, 0:2, :] = both[0:2, :]
    scc[r, 2:3, :] = row_sum
    for d in range(1, rows):
        scc_copy(d).start()
    root = lax.rsqrt(new_row)
    for d in range(1, rows):
        scc_copy(d).wait_recv()
    every = scc[0]
    for q in range(1, rows):
        every = every + scc[q]
    row_mean = every[2:3, :] / total_rows
    rms_update = jnp.sqrt(row_mean * (every[0:1, :] / entries))
    clip_factor = jnp.maximum(1.0, rms_update / CLIP_LIMIT)
    step_scale = STEP_SIZE * jnp.sqrt(every[1:2, :] / entries + MEAN_OFFSET)
    scale = step_scale / clip_factor * jnp.sqrt(row_mean)
    rs_out[...] = jnp.broadcast_to(root, (128, tile_rows)).T * scale

    @pl.loop(0, n)
    def _(j):
        own_x(j).wait_send()
        own_y(j).wait_send()
        fwd_y(j).wait_send()
        fwd_x(j).wait_send()
        for d in range(1, rows):
            col_copy(j, d).wait_send()

    @pl.loop(FIXED, n - SLOTS)
    def _(j):
        og_store(j).wait()

    for d in range(1, cols // 2):
        for copy in acts_copies(d):
            copy.wait_send()
    for d in range(cols // 2):
        for copy in sib_copies(d):
            copy.wait_send()
    for d in range(1, cols):
        row_copy(d).wait_send()
        scb_copy(d).wait_send()
    for d in range(1, rows):
        scc_copy(d).wait_send()


def update_kernel(og_ref, w_ref, rs_ref, cs_ref, *refs):
    acts_t, refs = refs[:PIECES], refs[PIECES:]
    grad, refs = refs[: PIECES * PARTS], refs[PIECES * PARTS :]
    out_ref, og_buf, made_buf, kept_buf, og_sem, in_sem, out_sem = refs
    n, _, width = og_ref.shape
    sub = acts_t[0].shape[0]
    thin = sub // PARTS
    narrow = width // SPLIT
    chunks = n - KEPT

    def og_load(t):
        return pltpu.make_async_copy(og_ref.at[FIXED + t], og_buf.at[lax.rem(t, OG_RING)], og_sem.at[lax.rem(t, OG_RING)])

    def copies(t, out):
        b = lax.rem(t, RING)
        made = pl.ds(pl.multiple_of((FIXED + t) * width, width), width)
        kept = pl.ds(pl.multiple_of(chunk_in(lax.div(t, SPLIT), n) * width + lax.rem(t, SPLIT) * narrow, narrow), narrow)
        if out:
            return (pltpu.make_async_copy(made_buf.at[b], out_ref.at[:, made], out_sem.at[0, b]),
                    pltpu.make_async_copy(kept_buf.at[b], out_ref.at[:, kept], out_sem.at[1, b]))
        return (pltpu.make_async_copy(w_ref.at[:, made], made_buf.at[b], in_sem.at[0, b]),
                pltpu.make_async_copy(w_ref.at[:, kept], kept_buf.at[b], in_sem.at[1, b]))

    def finish(g, w, row, cs):
        rs = rs_ref[pl.ds(row, g.shape[0]), :]
        wide = jnp.concatenate([rs] * (g.shape[1] // 128), axis=1)
        return (w.astype(jnp.float32) - g * wide * cs).astype(w.dtype)

    mixed = KEPT * SPLIT

    def each(t, out, act):
        made, kept = copies(t, out)
        act(made)

        @pl.when(t < mixed)
        def _():
            act(kept)

    def start(copy):
        copy.start()

    def wait(copy):
        copy.wait()

    for t in range(LOADS):
        og_load(t).start()
        each(t, False, start)

    def body(t, mix):
        b = lax.rem(t, RING)

        @pl.when(t >= RING - LOADS)
        def _():
            each(t - (RING - LOADS), True, wait)

        @pl.when(t + LOADS < chunks)
        def _():
            og_load(t + LOADS).start()
            each(t + LOADS, False, start)

        og_load(t).wait()
        each(t, False, wait)
        right = og_buf.at[lax.rem(t, OG_RING)]
        s = lax.div(t, SPLIT)
        lanes = pl.ds(pl.multiple_of(lax.rem(t, SPLIT) * narrow, narrow), narrow)
        made_cs = cs_ref[FIXED + t]
        kept_cs = cs_ref[chunk_in(s, n), :, lanes] if mix else None

        def make(row):
            i, low = row // sub, row % sub
            left = acts_t[i][low : low + ROWS, :]
            return row, jnp.dot(left, right[...], preferred_element_type=jnp.float32)

        def settle(row, g):
            at = pl.ds(row, ROWS)
            made_buf[b, at, :] = finish(g, made_buf[b, at, :], row, made_cs)

        def keep(p):
            at = pl.ds(p * thin, thin)
            kept_buf[b, at, :] = finish(grad[p][s, :, lanes], kept_buf[b, at, :], p * thin, kept_cs)

        blocks = sub * PIECES // ROWS
        parts = PIECES * PARTS
        last = None
        for k in range(blocks):
            g = make(k * ROWS)
            for p in range(k * parts // blocks, (k + 1) * parts // blocks) if mix else ():
                keep(p)
            if last is not None:
                settle(*last)
            last = g
        settle(*last)
        each(t, True, start)

    @pl.loop(0, mixed)
    def _(t):
        body(t, True)

    @pl.loop(mixed, chunks)
    def _(t):
        body(t, False)

    @pl.loop(chunks - (RING - LOADS), chunks)
    def _(t):
        each(t, True, wait)


def with_kernels(rows, cols, activations, output_grads, weight, row_moment, col_moment):
    tile_rows, tile_cols = weight.shape
    part = activations.shape[0]
    tokens = part * cols
    n, width = tile_cols // WIDTH, WIDTH
    f32, bf16 = jnp.float32, jnp.bfloat16
    any_space = pl.BlockSpec(memory_space=pl.ANY)
    vmem = pl.BlockSpec(memory_space=pltpu.VMEM)
    dma = pltpu.SemaphoreType.DMA
    flops = 2 * tile_rows * tile_cols * tokens
    sub = tile_rows // PIECES
    activations, output_grads, weight = (
        pltpu.with_memory_space_constraint(x, pltpu.HBM) for x in (activations, output_grads, weight))
    og_all, new_row, new_col, *inner = pl.pallas_call(
        functools.partial(gather_kernel, rows, cols),
        out_shape=(
            pltpu.HBM((n, tokens, width), bf16),
            jax.ShapeDtypeStruct((1, tile_rows), f32),
            jax.ShapeDtypeStruct((n, 1, width), f32),
            jax.ShapeDtypeStruct((tile_rows, 128), f32),
            jax.ShapeDtypeStruct((n, 1, width), f32),
            *([jax.ShapeDtypeStruct((sub, tokens), bf16)] * PIECES),
            *([jax.ShapeDtypeStruct((KEPT, sub // PARTS, width), f32)] * (PIECES * PARTS)),
        ),
        in_specs=[any_space, any_space, any_space, vmem, vmem],
        out_specs=(any_space,) + (vmem,) * (4 + PIECES + PIECES * PARTS),
        scratch_shapes=[
            pltpu.VMEM((n, tokens, width), bf16),
            pltpu.VMEM((W_RING, tile_rows // (n * WEIGHINGS), tile_cols), bf16),
            pltpu.VMEM((tile_rows, 128), f32),
            pltpu.VMEM((8, 1024), f32),
            pltpu.VMEM((rows, n, 1, width), f32),
            pltpu.VMEM((cols, 1, tile_rows), f32),
            pltpu.VMEM((cols, 2, 128), f32),
            pltpu.VMEM((rows, 3, 128), f32),
            dma((n,)), dma((2, 4, n)), dma((2, cols // 2, PIECES)), dma((2, cols // 2, PIECES)), dma((2, rows, n)),
            dma((2, cols)), dma((2, cols)), dma((2, rows)), dma((W_RING,)), dma((-(-tile_rows // width),)), dma((n,)),
        ],
        compiler_params=pltpu.CompilerParams(
            collective_id=0, has_side_effects=True, vmem_limit_bytes=GATHER_VMEM),
        cost_estimate=pl.CostEstimate(flops=flops, bytes_accessed=2 * weight.size, transcendentals=0),
        name="gather_stats",
    )(activations, output_grads, weight, row_moment.reshape(1, tile_rows), col_moment.reshape(n, 1, width))
    og_all = pltpu.with_memory_space_constraint(og_all, pltpu.HBM)
    new_weight = pl.pallas_call(
        update_kernel,
        out_shape=jax.ShapeDtypeStruct((tile_rows, tile_cols), bf16),
        in_specs=[any_space, any_space] + [vmem] * len(inner),
        out_specs=any_space,
        scratch_shapes=[
            pltpu.VMEM((OG_RING, tokens, width), bf16),
            pltpu.VMEM((RING, tile_rows, width), bf16),
            pltpu.VMEM((RING, tile_rows, width // SPLIT), bf16),
            dma((OG_RING,)), dma((2, RING)), dma((2, RING)),
        ],
        compiler_params=pltpu.CompilerParams(vmem_limit_bytes=UPDATE_VMEM),
        cost_estimate=pl.CostEstimate(flops=flops, bytes_accessed=4 * weight.size, transcendentals=0),
        name="update_weight",
    )(og_all, weight, *inner)
    return new_weight, new_row.reshape(tile_rows), new_col.reshape(tile_cols)


def plain(activations, output_grads, weight, row_moment, col_moment):
    tile_rows, tile_cols = weight.shape
    total_rows = tile_rows * lax.axis_size("row")
    total_cols = tile_cols * lax.axis_size("col")
    entries = float(total_rows * total_cols)
    weight_wide = weight.astype(jnp.float32)
    weight_local = jnp.sum(weight_wide * weight_wide)
    weight_total = lax.psum(weight_local, ("row", "col"))
    contract = (((0,), (0,)), ((), ()))
    acts_all = lax.all_gather(activations, "col", axis=0, tiled=True)
    gradient = lax.dot_general(
        acts_all,
        lax.all_gather(output_grads, "row", axis=0, tiled=True),
        contract,
        preferred_element_type=jnp.float32,
    )
    squared = gradient * gradient
    row_part = jnp.sum(squared + ADDED_SQUARE, axis=1)
    col_part = jnp.sum(squared + ADDED_SQUARE, axis=0)
    row_total = lax.psum(row_part, "col")
    col_total = lax.psum(col_part, "row")
    new_row = DECAY_RATE * row_moment + (1.0 - DECAY_RATE) * row_total / total_cols
    new_col = DECAY_RATE * col_moment + (1.0 - DECAY_RATE) * col_total / total_rows
    inverse = lax.rsqrt(new_row[:, None] * new_col[None, :])
    ratio_local = jnp.sum(squared * inverse * inverse)
    leader = (lax.axis_index("col") == 0).astype(jnp.float32)
    row_local = leader * jnp.sum(new_row)
    row_sum, ratio_sum = lax.psum((row_local, ratio_local), ("row", "col"))
    row_mean = row_sum / total_rows
    rms_update = jnp.sqrt(row_mean * ratio_sum / entries)
    clip_factor = jnp.maximum(1.0, rms_update / CLIP_LIMIT)
    step_scale = STEP_SIZE * jnp.sqrt(weight_total / entries + MEAN_OFFSET)
    update = gradient * inverse * jnp.sqrt(row_mean)
    new_weight = (weight_wide - step_scale / clip_factor * update).astype(jnp.bfloat16)
    return (new_weight, new_row, new_col)


def on_device(rows, cols, activations, output_grads, weight, row_moment, col_moment):
    tile_rows, tile_cols = weight.shape
    chunks = tile_cols // WIDTH
    fits = (
        rows == 4 and cols % 2 == 0 and cols > 2
        and tile_rows % (64 * PIECES * PARTS) == 0 and tile_rows % (PIECES * ROWS) == 0 and tile_cols % 1024 == 0
        and chunks > max(2 * ACTS_READY, KEPT + SLOTS) and tile_rows % (8 * chunks * WEIGHINGS) == 0
        and chunks >= KEPT * (SPLIT + 1) and tile_rows % ROWS == 0 and 2 * activations.shape[0] <= output_grads.shape[0]
        and output_grads.shape[0] % 32 == 0 and activations.shape[0] % 128 == 0
    )
    args = (activations, output_grads, weight, row_moment, col_moment)
    return with_kernels(rows, cols, *args) if fits else plain(*args)


def solution(mesh):
    return jax.shard_map(
        functools.partial(on_device, mesh.shape["row"], mesh.shape["col"]),
        mesh=mesh,
        in_specs=(P("col", "row"), P("row", "col"), P("row", "col"), P("row"), P("col")),
        out_specs=(P("row", "col"), P("row"), P("col")),
        check_vma=False,
    )
```
